256 devices in a mesh: groups: 4 (over x, y), dp: 64 (over z, core).
Axes of the slice: x: 2, y: 2, z: 32, core: 2. Of those that a mesh axis runs over, the one named last changes fastest.
The devices are a block of a 4x8x32 slice.
Arguments:
- tokens: bfloat16 [98304, 8192], P(('groups', 'dp')), parts along dimension 0, may hold values from -6 to 6
- base_weight: bfloat16 [8192, 768], P('dp'), may hold values from -0.0625 to 0.0625
- down_stack: bfloat16 [8192, 512], P('dp'), may hold values from -0.0625 to 0.0625
- up_stack: bfloat16 [512, 768], replicated, may hold values from -0.75 to 0.75
- adapter_scale: float32 [8], replicated, may hold values from 0.5 to 2
- lengths: int32 [512], P(('groups', 'dp')), parts along dimension 0, may hold values from 1 to 256, as said below
- adapter_ids: int32 [512], P(('groups', 'dp')), parts along dimension 0, may hold values from 0 to 7
Outputs:
- projected: bfloat16 [98304, 768], P(('groups', 'dp')), parts along dimension 0
The draws below stay inside these ranges and needn't reach their ends.
There are 4 independent parts, one for each index of `groups`. The reference program is written for one: setup_inputs(seed, part) draws one part's arguments, and reference() takes and returns one part's arrays. A program takes and returns all parts, laid end to end along the dimension named above; an argument that names none is the same for every part. Nothing has to cross between parts.
Inputs may be any that keep to these rules, and one draw needn't show every extreme that they name: `lengths`: each index of dp holds two requests whose block counts ceil(length / 128) add up to exactly 3.
All inputs are finite; a program needn't handle non-finite values.
Results may differ from the reference program's by a relative error of at most 0.0042.
Values may be sent and summed in bfloat16 or wider, within the bound.
No kernel may reach another device: no remote copies, remote signals or barrier semaphores. Data moves between devices by JAX's collectives and lax.ppermute only.
A program may use at most 128 MiB of HBM per device.

```python
import math
from functools import partial
import jax
import jax.numpy as jnp

D = 8192
RANK = 64
ADAPTERS = 8
BLOCK = 128
BLOCKS_DEV = 3
COLS = 768
TOK_DEV = 384
TOKENS = 24576
REQUESTS = 128
N_DP = 64


def draw_lengths(key, part):
    key_first, key_rest = jax.random.split(jax.random.fold_in(key, 11))
    pair_count = REQUESTS // 2
    first = jax.random.randint(key_first, (pair_count,), 1, BLOCKS_DEV)
    first = first.at[0].set(BLOCKS_DEV - 1)
    counts = jnp.stack([first, BLOCKS_DEV - first], axis=1)
    remainders = jax.random.randint(key_rest, (pair_count, 2), 1, BLOCK + 1)
    remainders = remainders.at[0, 0].set(BLOCK).at[0, 1].set(1)
    return ((counts - 1) * BLOCK + remainders).reshape(REQUESTS).astype(jnp.int32)


def touch_ends(array, own_key, low, top_value):
    longest = array.shape.index(max(array.shape))
    spots = []
    for shift in (0, 1):
        where = [jax.random.randint(jax.random.fold_in(own_key, axis), (), 0, length) for axis, length in enumerate(array.shape)]
        where[longest] = (where[longest] + shift) % array.shape[longest]
        spots.append(tuple(where))
    return array.at[spots[0]].set(low).at[spots[1]].set(top_value)


def levels(own_key, dims, cuts, low, top_value):
    loudness = 1.0
    for axis_at, blocks in cuts:
        steps = jax.random.uniform(jax.random.fold_in(jax.random.fold_in(own_key, 6), axis_at), (blocks,), jnp.float32, low / len(cuts), top_value / len(cuts))
        loudness = loudness * jnp.repeat(jnp.exp(steps), dims[axis_at] // blocks).reshape((-1,) + (1,) * (len(dims) - 1 - axis_at))
    return loudness


def noise(rng, extent, deviation, limit, cuts=(), kind=jnp.bfloat16):
    array = deviation * jax.random.normal(rng, extent, jnp.float32)
    if cuts:
        array = array * levels(rng, extent, cuts, -0.22, 0.18)
    return jnp.clip(array, -limit, limit).astype(kind)


def setup_inputs(seed: int = 0, part: int = 0) -> dict:
    keys = jax.random.split(jax.random.key(seed), 8)
    own_keys = jax.random.split(jax.random.fold_in(keys[7], part), 8)
    return {
        "tokens": noise(own_keys[0], (TOKENS, D), 1.0, 6.0, ((0, 64),)),
        "base_weight": noise(keys[1], (D, COLS), D ** -0.5, 0.0625, ((0, 64),)),
        "down_stack": noise(keys[2], (D, ADAPTERS * RANK), D ** -0.5, 0.0625, ((0, 64),)),
        "up_stack": noise(keys[3], (ADAPTERS * RANK, COLS), RANK ** -0.5, 0.75),
        "adapter_scale": jnp.clip(jnp.exp(jax.random.uniform(keys[4], (ADAPTERS,), jnp.float32, math.log(0.5), math.log(2.0))), 0.5, 2.0),
        "lengths": draw_lengths(jax.random.fold_in(jax.random.fold_in(keys[7], part), 71), part),
        "adapter_ids": touch_ends(jax.random.randint(own_keys[6], (REQUESTS,), 0, ADAPTERS), jax.random.fold_in(own_keys[6], 1), 0, ADAPTERS - 1).astype(jnp.int32),
    }


def layout(lengths, adapter_ids, row_count):
    counts = (lengths + BLOCK - 1) // BLOCK
    position = jnp.arange(row_count, dtype=jnp.int32)
    boundary = counts[0] * BLOCK
    second = position >= boundary
    offset = jnp.where(second, position - boundary, position)
    is_live = offset < jnp.where(second, lengths[1], lengths[0])
    token_adapter = jnp.where(second, adapter_ids[1], adapter_ids[0])
    return is_live, token_adapter.astype(jnp.int32)


def reference(tokens, base_weight, down_stack, up_stack, adapter_scale, lengths, adapter_ids):
    is_live, token_adapter = jax.vmap(partial(layout, row_count=TOK_DEV))(
        lengths.reshape(N_DP, 2), adapter_ids.reshape(N_DP, 2))
    is_live = is_live.reshape(-1)
    token_adapter = token_adapter.reshape(-1)
    base_out = jnp.dot(tokens, base_weight, preferred_element_type=jnp.float32)
    onehot = (token_adapter[:, None] == jnp.arange(ADAPTERS, dtype=jnp.int32)[None, :]).astype(jnp.float32)
    every_down_weight = jnp.dot(tokens, down_stack, preferred_element_type=jnp.float32).reshape(-1, ADAPTERS, RANK)
    low_rank = jnp.sum(onehot[:, :, None] * every_down_weight, axis=1).astype(jnp.bfloat16)
    widened = (onehot[:, :, None].astype(jnp.bfloat16) * low_rank[:, None, :]).reshape(-1, ADAPTERS * RANK)
    adapter_out = jnp.dot(widened, up_stack, preferred_element_type=jnp.float32)
    token_scale = jnp.sum(onehot * adapter_scale[None, :], axis=1)
    result = jnp.where(is_live[:, None], base_out + token_scale[:, None] * adapter_out, 0.0)
    return result.astype(jnp.bfloat16)
```

```python
import jax
import jax.numpy as jnp
from jax import lax
from jax.experimental import pallas as pl
from jax.experimental.pallas import tpu as pltpu
from jax.sharding import PartitionSpec as P

RANK = 64
BLOCK = 128
CORES = 2


def accumulate_kernel(n, first, block_ref, side_ref, tokens_ref, *refs):
    halves = refs[: 2 * n]
    acc_in = None if first else refs[2 * n]
    out_ref, tok, wide, sem = refs[2 * n + (0 if first else 1) :]
    copies = [
        pltpu.make_async_copy(
            tokens_ref.at[:, pl.ds(pl.multiple_of(block_ref[j] * BLOCK, BLOCK), BLOCK)],
            tok.at[:, j * BLOCK : (j + 1) * BLOCK],
            sem.at[j],
        )
        for j in range(n)
    ]
    for copy in copies:
        copy.start()
    half = halves[0].shape[0]
    for j in range(n):
        mine = pl.multiple_of(j * 2 * half + side_ref[j] * half, half)
        other = pl.multiple_of(j * 2 * half + (1 - side_ref[j]) * half, half)
        wide[pl.ds(mine, half), :] = halves[2 * j][...]
        wide[pl.ds(other, half), :] = halves[2 * j + 1][...]
    for copy in copies:
        copy.wait()
    step = 2 * BLOCK

    def column(k, carry):
        at = pl.ds(pl.multiple_of(k * step, step), step)
        part = jnp.dot(tok[...], wide[:, at], preferred_element_type=jnp.float32)
        out_ref[:, at] = part if first else acc_in[:, at] + part
        return carry

    lax.fori_loop(0, out_ref.shape[1] // step, column, 0)


def accumulate(acc, tokens, shards):
    n = len(shards)
    rows = tokens.shape[0]
    half, width = shards[0][0].shape
    blocks = jnp.stack([s[3] for s in shards]).astype(jnp.int32)
    sides = jnp.stack([s[2] for s in shards]).astype(jnp.int32)
    pieces = [a for s in shards for a in s[:2]]
    first = acc is None
    vmem = pl.BlockSpec(memory_space=pltpu.VMEM)
    smem = pl.BlockSpec(memory_space=pltpu.SMEM)
    return pl.pallas_call(
        lambda *refs: accumulate_kernel(n, first, *refs),
        out_shape=jax.ShapeDtypeStruct((rows, width), jnp.float32),
        in_specs=[smem, smem, pl.BlockSpec(memory_space=pl.ANY)] + [vmem] * (2 * n + (0 if first else 1)),
        out_specs=vmem,
        input_output_aliases={} if first else {3 + 2 * n: 0},
        scratch_shapes=[
            pltpu.VMEM((rows, n * BLOCK), jnp.bfloat16),
            pltpu.VMEM((n * 2 * half, width), jnp.bfloat16),
            pltpu.SemaphoreType.DMA((n,)),
        ],
        compiler_params=pltpu.CompilerParams(vmem_limit_bytes=24 * 2**20),
        cost_estimate=pl.CostEstimate(
            flops=2 * rows * n * BLOCK * width,
            bytes_accessed=2 * n * BLOCK * (rows + width) + 8 * rows * width,
            transcendentals=0,
        ),
    )(blocks, sides, tokens, *pieces, *([] if first else [acc]))


def finish_kernel(lengths_ref, ids_ref, scale_ref, acc_ref, got_ref, up_ref, out_ref):
    rows, cols = out_ref.shape
    deep = up_ref.shape[0]
    boundary = (lengths_ref[0] + BLOCK - 1) // BLOCK * BLOCK
    position = lax.broadcasted_iota(jnp.int32, (rows, 1), 0)
    second = position >= boundary
    offset = jnp.where(second, position - boundary, position)
    live = offset < jnp.where(second, lengths_ref[1], lengths_ref[0])
    adapter = jnp.where(second, ids_ref[1], ids_ref[0])
    scale = jnp.where(second, scale_ref[ids_ref[1]], scale_ref[ids_ref[0]])
    low = (acc_ref[:, cols:] + got_ref[:, cols:]).astype(jnp.bfloat16)
    owner = lax.broadcasted_iota(jnp.int32, (rows, deep), 1) // RANK
    wide = jnp.where(owner == adapter, low, jnp.zeros((), jnp.bfloat16))
    step = 2 * BLOCK
    for k in range(cols // step):
        at = slice(k * step, (k + 1) * step)
        extra = jnp.dot(wide, up_ref[:, at], preferred_element_type=jnp.float32)
        base = acc_ref[:, at] + got_ref[:, at]
        out_ref[:, at] = jnp.where(live, base + scale * extra, 0.0).astype(out_ref.dtype)


def finish(acc, got, up, scale, lengths, ids):
    vmem = pl.BlockSpec(memory_space=pltpu.VMEM)
    smem = pl.BlockSpec(memory_space=pltpu.SMEM)
    rows, width = acc.shape
    deep, cols = up.shape
    return pl.pallas_call(
        finish_kernel,
        out_shape=jax.ShapeDtypeStruct((rows, cols), jnp.bfloat16),
        in_specs=[smem, smem, smem, vmem, vmem, vmem],
        out_specs=vmem,
        compiler_params=pltpu.CompilerParams(vmem_limit_bytes=24 * 2**20),
        cost_estimate=pl.CostEstimate(flops=2 * rows * deep * cols, bytes_accessed=8 * rows * width, transcendentals=0),
    )(lengths, ids, scale, acc, got, up)


def plan(far):
    edges = [0, 4, 8, 12, 14, far]
    return [range(lo + (1 if k else 0), hi + 1) for k, (lo, hi) in enumerate(zip(edges, edges[1:]))]


def solution(mesh):
    dp = mesh.shape["dp"]
    groups = mesh.shape["groups"]
    chips = dp // CORES
    far = chips // 2
    first_x = [d.coords[0] for d in mesh.devices[:, 0]]
    per_x = first_x.count(first_x[0])
    forth = [(i, (i + CORES) % dp) for i in range(dp)]
    back = [(i, (i - CORES) % dp) for i in range(dp)]
    mate = [(i, i ^ 1) for i in range(dp)]
    over_y = [(i, i ^ 1) for i in range(groups)]
    over_x = [(i, i ^ per_x) for i in range(groups)]

    def local(tokens, base_weight, down_stack, up_stack, adapter_scale, lengths, adapter_ids):
        place = lax.axis_index("dp")
        group = lax.axis_index("groups")
        chip, core = place // CORES, place % CORES
        side_x, side_y = (group // per_x) % 2, group % 2
        own = jnp.concatenate([base_weight, down_stack], axis=1)
        half = own.shape[0] // 2
        f = lax.dynamic_slice_in_dim(own, side_x * half, half, 0)
        b = lax.dynamic_slice_in_dim(own, side_y * half, half, 0)
        zero = jnp.zeros((), jnp.int32)
        got = {0: [(own[:half], own[half:], zero, place)]}
        theirs = lax.ppermute(tokens, "dp", mate)
        for s in range(1, far + 1):
            f = lax.ppermute(f, "dp", forth)
            fx = lax.ppermute(f, "groups", over_x)
            got[s] = [(f, fx, side_x, (chip - s) % chips * CORES + core)]
            if s < chips - far:
                b = lax.ppermute(b, "dp", back)
                by = lax.ppermute(b, "groups", over_y)
                got[s].append((b, by, side_y, (chip + s) % chips * CORES + core))
        acc = acc_theirs = None
        for steps in plan(far):
            shards = [x for s in steps for x in got[s]]
            acc_theirs = accumulate(acc_theirs, theirs, shards)
            acc = accumulate(acc, tokens, shards)
        rest = lax.ppermute(acc_theirs, "dp", mate)
        return finish(acc, rest, up_stack, adapter_scale, lengths, adapter_ids)

    in_specs = (
        P(("groups", "dp"), None),
        P("dp", None),
        P("dp", None),
        P(),
        P(),
        P(("groups", "dp")),
        P(("groups", "dp")),
    )
    return jax.shard_map(local, mesh=mesh, in_specs=in_specs, out_specs=P(("groups", "dp"), None), check_vma=False)
```

```python
import jax
import jax.numpy as jnp
from jax import lax
from jax.experimental import pallas as pl
from jax.experimental.pallas import tpu as pltpu
from jax.sharding import PartitionSpec as P

RANK = 64
BLOCK = 128
CORES = 2
TILE = 256

VMEM = pl.BlockSpec(memory_space=pltpu.VMEM)
SMEM = pl.BlockSpec(memory_space=pltpu.SMEM)
ANY = pl.BlockSpec(memory_space=pl.ANY)
LIMIT = 20 * 2**20


def side_by_side_kernel(left_ref, right_ref, top_ref, low_ref):
    half, cut = top_ref.shape[0], left_ref.shape[1]
    top_ref[:, :cut] = left_ref[:half, :]
    top_ref[:, cut:] = right_ref[:half, :]
    low_ref[:, :cut] = left_ref[half:, :]
    low_ref[:, cut:] = right_ref[half:, :]


def side_by_side(left, right):
    shape = jax.ShapeDtypeStruct((left.shape[0] // 2, left.shape[1] + right.shape[1]), left.dtype)
    return pl.pallas_call(
        side_by_side_kernel,
        out_shape=[shape, shape],
        in_specs=[VMEM, VMEM],
        out_specs=[VMEM, VMEM],
        compiler_params=pltpu.CompilerParams(vmem_limit_bytes=LIMIT),
    )(left, right)


def stack_kernel(*refs):
    rows = refs[0].shape[0]
    for k, ref in enumerate(refs[:-1]):
        refs[-1][k * rows : (k + 1) * rows, :] = ref[...]


def stack(pieces):
    rows, width = pieces[0].shape
    return pl.pallas_call(
        stack_kernel,
        out_shape=jax.ShapeDtypeStruct((rows * len(pieces), width), pieces[0].dtype),
        in_specs=[VMEM] * len(pieces),
        out_specs=VMEM,
        compiler_params=pltpu.CompilerParams(vmem_limit_bytes=LIMIT),
        cost_estimate=pl.CostEstimate(flops=2**20, bytes_accessed=4 * rows * width * len(pieces), transcendentals=0),
    )(*pieces)


def accumulate_kernel(sources, part_count, first, chips, where_ref, tokens_ref, *refs):
    parts = refs[:part_count]
    acc_in = None if first else refs[part_count]
    out_ref, tok, sem = refs[part_count + (0 if first else 1) :]
    chip, sign, core = where_ref[0], where_ref[1], where_ref[2]
    copies = []
    for k, (distance, mine) in enumerate(sources):
        source = lax.rem(chip + sign * distance + chips, chips)
        column = (source * CORES + (core if mine else 1 - core)) * BLOCK
        copies.append(
            pltpu.make_async_copy(
                tokens_ref.at[:, pl.ds(pl.multiple_of(column, BLOCK), BLOCK)],
                tok.at[:, k * BLOCK : (k + 1) * BLOCK],
                sem.at[k],
            )
        )
    for copy in copies:
        copy.start()
    for copy in copies:
        copy.wait()

    def column_tile(k, carry):
        at = pl.ds(pl.multiple_of(k * TILE, TILE), TILE)
        total = None if first else acc_in[:, at]
        begin = 0
        for part in parts:
            end = begin + part.shape[0]
            term = jnp.dot(tok[:, begin:end], part[:, at], preferred_element_type=jnp.float32)
            total = term if total is None else total + term
            begin = end
        out_ref[:, at] = total
        return carry

    lax.fori_loop(0, out_ref.shape[1] // TILE, column_tile, 0)


def accumulate(acc, tokens, where, chips, sources, parts):
    rows, width = tokens.shape[0], parts[0].shape[1]
    first = acc is None
    n = len(sources)
    return pl.pallas_call(
        lambda *refs: accumulate_kernel(sources, len(parts), first, chips, *refs),
        out_shape=jax.ShapeDtypeStruct((rows, width), jnp.float32),
        in_specs=[SMEM, ANY] + [VMEM] * (len(parts) + (0 if first else 1)),
        out_specs=VMEM,
        input_output_aliases={} if first else {2 + len(parts): 0},
        scratch_shapes=[pltpu.VMEM((rows, n * BLOCK), jnp.bfloat16), pltpu.SemaphoreType.DMA((n,))],
        compiler_params=pltpu.CompilerParams(vmem_limit_bytes=LIMIT),
        cost_estimate=pl.CostEstimate(
            flops=2 * rows * n * BLOCK * width,
            bytes_accessed=2 * n * BLOCK * (rows + width) + 8 * rows * width,
            transcendentals=0,
        ),
    )(where, tokens, *parts, *([] if first else [acc]))


def finish_kernel(lengths_ref, ids_ref, scale_ref, acc_ref, got_ref, up_ref, out_ref):
    rows, cols = out_ref.shape
    deep = up_ref.shape[0]
    boundary = (lengths_ref[0] + BLOCK - 1) // BLOCK * BLOCK
    position = lax.broadcasted_iota(jnp.int32, (rows, 1), 0)
    second = position >= boundary
    offset = jnp.where(second, position - boundary, position)
    live = offset < jnp.where(second, lengths_ref[1], lengths_ref[0])
    adapter = jnp.where(second, ids_ref[1], ids_ref[0])
    scale = jnp.where(second, scale_ref[ids_ref[1]], scale_ref[ids_ref[0]])
    low = (acc_ref[:, cols:] + got_ref[:, cols:]).astype(jnp.bfloat16)
    owner = lax.broadcasted_iota(jnp.int32, (rows, deep), 1) // RANK
    wide = jnp.where(owner == adapter, low, jnp.zeros((), jnp.bfloat16))
    for k in range(cols // TILE):
        at = slice(k * TILE, (k + 1) * TILE)
        extra = jnp.dot(wide, up_ref[:, at], preferred_element_type=jnp.float32)
        base = acc_ref[:, at] + got_ref[:, at]
        out_ref[:, at] = jnp.where(live, base + scale * extra, 0.0).astype(out_ref.dtype)


def finish(acc, got, up, scale, lengths, ids):
    rows, width = acc.shape
    deep, cols = up.shape
    return pl.pallas_call(
        finish_kernel,
        out_shape=jax.ShapeDtypeStruct((rows, cols), jnp.bfloat16),
        in_specs=[SMEM, SMEM, SMEM, VMEM, VMEM, VMEM],
        out_specs=VMEM,
        compiler_params=pltpu.CompilerParams(vmem_limit_bytes=LIMIT),
        cost_estimate=pl.CostEstimate(flops=2 * rows * deep * cols, bytes_accessed=8 * rows * width, transcendentals=0),
    )(lengths, ids, scale, acc, got, up)


BATCHES = ((1, 2), (3, 5), (6, 8), (9, 11), (12, 13), (14, 15))


def solution(mesh):
    dp = mesh.shape["dp"]
    groups = mesh.shape["groups"]
    chips = dp // CORES
    far = chips // 2
    first_x = [d.coords[0] for d in mesh.devices[:, 0]]
    per_x = first_x.count(first_x[0])

    def parity(g):
        return (g // per_x + g % per_x) % 2

    def flat(g, z, c):
        return g * dp + z % chips * CORES + c

    places = [(g, z, c) for g in range(groups) for z in range(chips) for c in range(CORES)]
    along = [(flat(g, z, c), flat(g, z + (1 if c == parity(g) else -1), c)) for g, z, c in places]
    across = [(flat(g, z, c), flat(g ^ per_x if c == parity(g) else g ^ 1, z, 1 - c)) for g, z, c in places]
    mate = [(i, i ^ 1) for i in range(dp)]
    both = ("groups", "dp")

    def local(tokens, base_weight, down_stack, up_stack, adapter_scale, lengths, adapter_ids):
        place = lax.axis_index("dp")
        group = lax.axis_index("groups")
        chip, core = place // CORES, place % CORES
        sign = jnp.where(core == parity(group), -1, 1)
        where = jnp.stack([chip, sign, core]).astype(jnp.int32)
        own = side_by_side(base_weight, down_stack)
        theirs = lax.ppermute(tokens, "dp", mate)
        a, b = own
        pieces = {}
        for s in range(1, far + 1):
            a = lax.ppermute(a, both, along)
            b = lax.ppermute(b, both, along)
            pieces[s] = [a, b]
        acc = acc_theirs = None
        for k, (lo, hi) in enumerate(BATCHES):
            steps = range(lo, hi + 1)
            near = stack([p for s in steps for p in pieces[s]])
            parts = [near, lax.ppermute(near, both, across)]
            sources = [(s, True) for s in steps] + [(s, False) for s in steps]
            if k == len(BATCHES) - 1:
                parts += [*own, *pieces[far]]
                sources += [(0, True), (far, True)]
            acc_theirs = accumulate(acc_theirs, theirs, where, chips, sources, parts)
            acc = accumulate(acc, tokens, where, chips, sources, parts)
        rest = lax.ppermute(acc_theirs, "dp", mate)
        return finish(acc, rest, up_stack, adapter_scale, lengths, adapter_ids)

    in_specs = (
        P(("groups", "dp"), None),
        P("dp", None),
        P("dp", None),
        P(),
        P(),
        P(("groups", "dp")),
        P(("groups", "dp")),
    )
    return jax.shard_map(local, mesh=mesh, in_specs=in_specs, out_specs=P(("groups", "dp"), None), check_vma=False)
```

```python
import jax
import jax.numpy as jnp
from jax import lax
from jax.experimental import pallas as pl
from jax.experimental.pallas import tpu as pltpu
from jax.sharding import PartitionSpec as P

RANK = 64
BLOCK = 128
CORES = 2
TILE = 256

VMEM = pl.BlockSpec(memory_space=pltpu.VMEM)
SMEM = pl.BlockSpec(memory_space=pltpu.SMEM)
ANY = pl.BlockSpec(memory_space=pl.ANY)
LIMIT = 20 * 2**20


def side_by_side_kernel(left_ref, right_ref, whole_ref, top_ref, low_ref):
    half, cut = top_ref.shape[0], left_ref.shape[1]
    whole_ref[:, :cut] = left_ref[...]
    whole_ref[:, cut:] = right_ref[...]
    top_ref[:, :cut] = left_ref[:half, :]
    top_ref[:, cut:] = right_ref[:half, :]
    low_ref[:, :cut] = left_ref[half:, :]
    low_ref[:, cut:] = right_ref[half:, :]


def side_by_side(left, right):
    rows, width = left.shape[0], left.shape[1] + right.shape[1]
    whole = jax.ShapeDtypeStruct((rows, width), left.dtype)
    half = jax.ShapeDtypeStruct((rows // 2, width), left.dtype)
    return pl.pallas_call(
        side_by_side_kernel,
        out_shape=[whole, half, half],
        in_specs=[VMEM, VMEM],
        out_specs=[VMEM] * 3,
        compiler_params=pltpu.CompilerParams(vmem_limit_bytes=LIMIT),
    )(left, right)


def stack_kernel(steps, where_ref, *refs):
    out_ref = refs[-1]
    rows = refs[0].shape[0]
    for k, s in enumerate(steps):
        first = lax.rem(where_ref[0] + s, 2) == 0
        for j in range(2):
            at = slice((2 * k + j) * rows, (2 * k + j + 1) * rows)
            one, two = refs[4 * k + j], refs[4 * k + 2 + j]

            @pl.when(first)
            def _():
                out_ref[at, :] = one[...]

            @pl.when(jnp.logical_not(first))
            def _():
                out_ref[at, :] = two[...]


def stack(where, steps, pieces):
    rows, width = pieces[0].shape
    return pl.pallas_call(
        lambda *refs: stack_kernel(steps, *refs),
        out_shape=jax.ShapeDtypeStruct((rows * len(pieces) // 2, width), pieces[0].dtype),
        in_specs=[SMEM] + [VMEM] * len(pieces),
        out_specs=VMEM,
        compiler_params=pltpu.CompilerParams(vmem_limit_bytes=LIMIT),
        cost_estimate=pl.CostEstimate(flops=2**20, bytes_accessed=4 * rows * width * len(pieces), transcendentals=0),
    )(where, *pieces)


def accumulate_kernel(sources, part_count, token_count, base_row, chips, where_ref, *refs):
    tokens = refs[:token_count]
    parts = refs[token_count : token_count + part_count]
    out_ref, tok, sem = refs[-3:]
    acc_in = refs[token_count + part_count] if len(refs) > token_count + part_count + 3 else None
    rows = tokens[0].shape[0]
    chip, sign, core = where_ref[0], where_ref[1], where_ref[2]
    copies = []
    for k, (distance, mine) in enumerate(sources):
        source = lax.rem(chip + sign * distance + chips, chips)
        column = (source * CORES + (core if mine else 1 - core)) * BLOCK
        for t, tokens_ref in enumerate(tokens):
            copies.append(
                pltpu.make_async_copy(
                    tokens_ref.at[:, pl.ds(pl.multiple_of(column, BLOCK), BLOCK)],
                    tok.at[t * rows : (t + 1) * rows, k * BLOCK : (k + 1) * BLOCK],
                    sem.at[k, t],
                )
            )
    for copy in copies:
        copy.start()
    for copy in copies:
        copy.wait()

    def column_tile(k, carry):
        at = pl.ds(pl.multiple_of(k * TILE, TILE), TILE)
        total = None if acc_in is None else acc_in[base_row : base_row + tok.shape[0], at]
        begin = 0
        for part in parts:
            end = begin + part.shape[0]
            term = jnp.dot(tok[:, begin:end], part[:, at], preferred_element_type=jnp.float32)
            total = term if total is None else total + term
            begin = end
        out_ref[:, at] = total
        return carry

    lax.fori_loop(0, out_ref.shape[1] // TILE, column_tile, 0)


def accumulate(acc, tokens, where, chips, sources, parts, base_row=0):
    rows, width = tokens[0].shape[0] * len(tokens), parts[0].shape[1]
    n = len(sources)
    whole = acc is not None and acc.shape[0] == rows
    return pl.pallas_call(
        lambda *refs: accumulate_kernel(sources, len(parts), len(tokens), base_row, chips, *refs),
        out_shape=jax.ShapeDtypeStruct((rows, width), jnp.float32),
        in_specs=[SMEM] + [ANY] * len(tokens) + [VMEM] * (len(parts) + (acc is not None)),
        out_specs=VMEM,
        input_output_aliases={1 + len(tokens) + len(parts): 0} if whole else {},
        scratch_shapes=[pltpu.VMEM((rows, n * BLOCK), jnp.bfloat16), pltpu.SemaphoreType.DMA((n, len(tokens)))],
        compiler_params=pltpu.CompilerParams(vmem_limit_bytes=LIMIT),
        cost_estimate=pl.CostEstimate(
            flops=2 * rows * n * BLOCK * width,
            bytes_accessed=2 * n * BLOCK * (rows + width) + 8 * rows * width,
            transcendentals=0,
        ),
    )(where, *tokens, *parts, *([] if acc is None else [acc]))


def finish_kernel(lengths_ref, ids_ref, scale_ref, acc_ref, got_ref, up_ref, out_ref):
    rows, cols = out_ref.shape
    deep = up_ref.shape[0]
    boundary = (lengths_ref[0] + BLOCK - 1) // BLOCK * BLOCK
    position = lax.broadcasted_iota(jnp.int32, (rows, 1), 0)
    second = position >= boundary
    offset = jnp.where(second, position - boundary, position)
    live = offset < jnp.where(second, lengths_ref[1], lengths_ref[0])
    adapter = jnp.where(second, ids_ref[1], ids_ref[0])
    scale = jnp.where(second, scale_ref[ids_ref[1]], scale_ref[ids_ref[0]])
    low = (acc_ref[:, cols:] + got_ref[:, cols:]).astype(jnp.bfloat16)
    owner = lax.broadcasted_iota(jnp.int32, (rows, deep), 1) // RANK
    wide = jnp.where(owner == adapter, low, jnp.zeros((), jnp.bfloat16))
    for k in range(cols // TILE):
        at = slice(k * TILE, (k + 1) * TILE)
        extra = jnp.dot(wide, up_ref[:, at], preferred_element_type=jnp.float32)
        base = acc_ref[:, at] + got_ref[:, at]
        out_ref[:, at] = jnp.where(live, base + scale * extra, 0.0).astype(out_ref.dtype)


def finish(acc, got, up, scale, lengths, ids):
    rows, width = acc.shape
    deep, cols = up.shape
    return pl.pallas_call(
        finish_kernel,
        out_shape=jax.ShapeDtypeStruct((rows, cols), jnp.bfloat16),
        in_specs=[SMEM, SMEM, SMEM, VMEM, VMEM, VMEM],
        out_specs=VMEM,
        compiler_params=pltpu.CompilerParams(vmem_limit_bytes=LIMIT),
        cost_estimate=pl.CostEstimate(flops=2 * rows * deep * cols, bytes_accessed=8 * rows * width, transcendentals=0),
    )(lengths, ids, scale, acc, got, up)


BATCHES = ((1, 2), (3, 5), (6, 8), (9, 11), (12, 13), (14, 15))


def solution(mesh):
    dp = mesh.shape["dp"]
    groups = mesh.shape["groups"]
    chips = dp // CORES
    far = chips // 2
    first_x = [d.coords[0] for d in mesh.devices[:, 0]]
    per_x = first_x.count(first_x[0])

    def parity(g):
        return (g // per_x + g % per_x) % 2

    def flat(g, z, c):
        return g * dp + z % chips * CORES + c

    places = [(g, z, c) for g in range(groups) for z in range(chips) for c in range(CORES)]
    along = [
        [(flat(g, z, c), flat(g, z + (1 if c == parity(g) else -1), c)) for g, z, c in places if z % 2 == odd]
        for odd in range(2)
    ]
    across = [(flat(g, z, c), flat(g ^ per_x if c == parity(g) else g ^ 1, z, 1 - c)) for g, z, c in places]
    mate = [(i, i ^ 1) for i in range(dp)]
    both = ("groups", "dp")

    def local(tokens, base_weight, down_stack, up_stack, adapter_scale, lengths, adapter_ids):
        place = lax.axis_index("dp")
        group = lax.axis_index("groups")
        chip, core = place // CORES, place % CORES
        sign = jnp.where(core == parity(group), -1, 1)
        where = jnp.stack([chip, sign, core]).astype(jnp.int32)
        own, top, low = side_by_side(base_weight, down_stack)
        theirs = lax.ppermute(tokens, "dp", mate)
        waves = [top, top, low, low]
        pieces = {}
        for s in range(1, far + 1):
            waves = [lax.ppermute(x, both, along[(s + 1 + k) % 2]) for k, x in enumerate(waves)]
            pieces[s] = [waves[0], waves[2], waves[1], waves[3]]
        acc = None
        last = len(BATCHES) - 1
        for k, (lo, hi) in enumerate(BATCHES):
            steps = range(lo, hi + 1)
            near = stack(where, steps, [p for s in steps for p in pieces[s]])
            parts = [near, lax.ppermute(near, both, across)]
            sources = [(s, True) for s in steps] + [(s, False) for s in steps]
            if k == 0:
                parts.append(own)
                sources.append((0, True))
            if k < last:
                acc = accumulate(acc, [tokens, theirs], where, chips, sources, parts)
        parts.append(stack(where, [far], pieces[far]))
        sources.append((far, True))
        acc_theirs = accumulate(acc, [theirs], where, chips, sources, parts, tokens.shape[0])
        rest = lax.ppermute(acc_theirs, "dp", mate)
        acc = accumulate(acc, [tokens], where, chips, sources, parts)
        return finish(acc, rest, up_stack, adapter_scale, lengths, adapter_ids)

    in_specs = (
        P(("groups", "dp"), None),
        P("dp", None),
        P("dp", None),
        P(),
        P(),
        P(("groups", "dp")),
        P(("groups", "dp")),
    )
    return jax.shard_map(local, mesh=mesh, in_specs=in_specs, out_specs=P(("groups", "dp"), None), check_vma=False)
```

```python
import jax
import jax.numpy as jnp
from jax import lax
from jax.experimental import pallas as pl
from jax.experimental.pallas import tpu as pltpu
from jax.sharding import PartitionSpec as P

RANK = 64
BLOCK = 128
CORES = 2
TILE = 256

VMEM = pl.BlockSpec(memory_space=pltpu.VMEM)
SMEM = pl.BlockSpec(memory_space=pltpu.SMEM)
ANY = pl.BlockSpec(memory_space=pl.ANY)
LIMIT = 20 * 2**20


def side_by_side_kernel(left_ref, right_ref, whole_ref, top_ref, low_ref, sem):
    half, cut = top_ref.shape[0], left_ref.shape[1]
    copies = []
    for ref, rows in ((top_ref, slice(0, half)), (low_ref, slice(half, 2 * half)), (whole_ref, slice(0, 2 * half))):
        for source, columns in ((left_ref, slice(0, cut)), (right_ref, slice(cut, whole_ref.shape[1]))):
            copies.append(
                pltpu.make_async_copy(source.at[rows, :], ref.at[:, columns], sem.at[len(copies)])
            )
    for copy in copies:
        copy.start()
    for copy in copies:
        copy.wait()


def side_by_side(left, right):
    rows, width = left.shape[0], left.shape[1] + right.shape[1]
    whole = jax.ShapeDtypeStruct((rows, width), left.dtype)
    half = jax.ShapeDtypeStruct((rows // 2, width), left.dtype)
    return pl.pallas_call(
        side_by_side_kernel,
        out_shape=[whole, half, half],
        in_specs=[pl.BlockSpec(memory_space=pltpu.HBM)] * 2,
        out_specs=[VMEM] * 3,
        scratch_shapes=[pltpu.SemaphoreType.DMA((6,))],
        compiler_params=pltpu.CompilerParams(vmem_limit_bytes=LIMIT),
    )(left, right)


def stack_kernel(*refs):
    rows = refs[0].shape[0]
    for k, ref in enumerate(refs[:-1]):
        refs[-1][k * rows : (k + 1) * rows, :] = ref[...]


def stack(pieces):
    rows, width = pieces[0].shape
    return pl.pallas_call(
        stack_kernel,
        out_shape=jax.ShapeDtypeStruct((rows * len(pieces), width), pieces[0].dtype),
        in_specs=[VMEM] * len(pieces),
        out_specs=VMEM,
        compiler_params=pltpu.CompilerParams(vmem_limit_bytes=LIMIT),
        cost_estimate=pl.CostEstimate(flops=2**20, bytes_accessed=4 * rows * width * len(pieces), transcendentals=0),
    )(*pieces)


def accumulate_kernel(sources, part_count, first, chips, where_ref, tokens_ref, *refs):
    parts = refs[:part_count]
    acc_in = None if first else refs[part_count]
    out_ref, tok, sem = refs[part_count + (0 if first else 1) :]
    chip, sign, core = where_ref[0], where_ref[1], where_ref[2]
    copies = []
    for k, (distance, mine) in enumerate(sources):
        source = lax.rem(chip + sign * distance + chips, chips)
        side = lax.rem(core + distance + (0 if mine else 1), CORES)
        column = (source * CORES + side) * BLOCK
        copies.append(
            pltpu.make_async_copy(
                tokens_ref.at[:, pl.ds(pl.multiple_of(column, BLOCK), BLOCK)],
                tok.at[:, k * BLOCK : (k + 1) * BLOCK],
                sem.at[k],
            )
        )
    for copy in copies:
        copy.start()
    for copy in copies:
        copy.wait()

    def column_tile(k, carry):
        at = pl.ds(pl.multiple_of(k * TILE, TILE), TILE)
        total = None if first else acc_in[:, at]
        begin = 0
        for part in parts:
            end = begin + part.shape[0]
            term = jnp.dot(tok[:, begin:end], part[:, at], preferred_element_type=jnp.float32)
            total = term if total is None else total + term
            begin = end
        out_ref[:, at] = total.astype(out_ref.dtype)
        return carry

    lax.fori_loop(0, out_ref.shape[1] // TILE, column_tile, 0)


def accumulate(acc, tokens, where, chips, sources, parts, dtype=jnp.float32):
    rows, width = tokens.shape[0], parts[0].shape[1]
    first = acc is None
    n = len(sources)
    return pl.pallas_call(
        lambda *refs: accumulate_kernel(sources, len(parts), first, chips, *refs),
        out_shape=jax.ShapeDtypeStruct((rows, width), dtype),
        in_specs=[SMEM, ANY] + [VMEM] * (len(parts) + (0 if first else 1)),
        out_specs=VMEM,
        input_output_aliases={} if first or dtype != acc.dtype else {2 + len(parts): 0},
        scratch_shapes=[pltpu.VMEM((rows, n * BLOCK), jnp.bfloat16), pltpu.SemaphoreType.DMA((n,))],
        compiler_params=pltpu.CompilerParams(vmem_limit_bytes=LIMIT),
        cost_estimate=pl.CostEstimate(
            flops=2 * rows * n * BLOCK * width,
            bytes_accessed=2 * n * BLOCK * (rows + width) + 8 * rows * width,
            transcendentals=0,
        ),
    )(where, tokens, *parts, *([] if first else [acc]))


def finish_kernel(lengths_ref, ids_ref, scale_ref, acc_ref, got_ref, up_ref, out_ref):
    rows, cols = out_ref.shape
    deep = up_ref.shape[0]
    boundary = (lengths_ref[0] + BLOCK - 1) // BLOCK * BLOCK
    position = lax.broadcasted_iota(jnp.int32, (rows, 1), 0)
    second = position >= boundary
    offset = jnp.where(second, position - boundary, position)
    live = offset < jnp.where(second, lengths_ref[1], lengths_ref[0])
    adapter = jnp.where(second, ids_ref[1], ids_ref[0])
    scale = jnp.where(second, scale_ref[ids_ref[1]], scale_ref[ids_ref[0]])
    low = (acc_ref[:, cols:] + got_ref[:, cols:].astype(jnp.float32)).astype(jnp.bfloat16)
    owner = lax.broadcasted_iota(jnp.int32, (rows, deep), 1) // RANK
    wide = jnp.where(owner == adapter, low, jnp.zeros((), jnp.bfloat16))
    for k in range(cols // TILE):
        at = slice(k * TILE, (k + 1) * TILE)
        extra = jnp.dot(wide, up_ref[:, at], preferred_element_type=jnp.float32)
        base = acc_ref[:, at] + got_ref[:, at].astype(jnp.float32)
        out_ref[:, at] = jnp.where(live, base + scale * extra, 0.0).astype(out_ref.dtype)


def finish(acc, got, up, scale, lengths, ids):
    rows, width = acc.shape
    deep, cols = up.shape
    return pl.pallas_call(
        finish_kernel,
        out_shape=jax.ShapeDtypeStruct((rows, cols), jnp.bfloat16),
        in_specs=[SMEM, SMEM, SMEM, VMEM, VMEM, VMEM],
        out_specs=VMEM,
        compiler_params=pltpu.CompilerParams(vmem_limit_bytes=LIMIT),
        cost_estimate=pl.CostEstimate(flops=2 * rows * deep * cols, bytes_accessed=8 * rows * width, transcendentals=0),
    )(lengths, ids, scale, acc, got, up)


BATCHES = ((1, 2), (3, 5), (6, 8), (9, 11), (12, 13), (14, 15))


def solution(mesh):
    dp = mesh.shape["dp"]
    groups = mesh.shape["groups"]
    chips = dp // CORES
    far = chips // 2
    first_x = [d.coords[0] for d in mesh.devices[:, 0]]
    per_x = first_x.count(first_x[0])

    def parity(g):
        return (g // per_x + g % per_x) % 2

    def flat(g, z, c):
        return g * dp + z % chips * CORES + c

    places = [(g, z, c) for g in range(groups) for z in range(chips) for c in range(CORES)]
    forth = {(g, z, c): c == (parity(g) + z) % CORES for g, z, c in places}
    along = [(flat(*p), flat(p[0], p[1] + (1 if forth[p] else -1), 1 - p[2])) for p in places]
    across = [(flat(*p), flat(p[0] ^ per_x if forth[p] else p[0] ^ 1, p[1], 1 - p[2])) for p in places]
    mate = [(i, i ^ 1) for i in range(dp)]
    both = ("groups", "dp")

    def local(tokens, base_weight, down_stack, up_stack, adapter_scale, lengths, adapter_ids):
        place = lax.axis_index("dp")
        group = lax.axis_index("groups")
        chip, core = place // CORES, place % CORES
        sign = jnp.where(core == (parity(group) + chip) % CORES, -1, 1)
        where = jnp.stack([chip, sign, core]).astype(jnp.int32)
        own, a, b = side_by_side(base_weight, down_stack)
        theirs = lax.ppermute(tokens, "dp", mate)
        pieces = {}
        for s in range(1, far + 1):
            a = lax.ppermute(a, both, along)
            b = lax.ppermute(b, both, along)
            pieces[s] = [a, b]
        acc = acc_theirs = None
        last = len(BATCHES) - 1
        for k, (lo, hi) in enumerate(BATCHES):
            steps = range(lo, hi + 1)
            near = stack([p for s in steps for p in pieces[s]])
            got = lax.ppermute(near, both, across)
            parts, sources = [near], [(s, True) for s in steps]
            other = [(s, False) for s in steps]
            if k < last:
                parts, sources = parts + [got], sources + other
            if k == 0:
                parts, sources = parts + [own], sources + [(0, True)]
            if k == last:
                parts, sources = parts + [stack(pieces[far])], sources + [(far, True)]
            acc_theirs = accumulate(acc_theirs, theirs, where, chips, sources, parts)
            acc = accumulate(acc, tokens, where, chips, sources, parts)
        acc_theirs = accumulate(acc_theirs, theirs, where, chips, other, [got], jnp.bfloat16)
        rest = lax.ppermute(acc_theirs, "dp", mate)
        acc = accumulate(acc, tokens, where, chips, other, [got])
        return finish(acc, rest, up_stack, adapter_scale, lengths, adapter_ids)

    in_specs = (
        P(("groups", "dp"), None),
        P("dp", None),
        P("dp", None),
        P(),
        P(),
        P(("groups", "dp")),
        P(("groups", "dp")),
    )
    return jax.shard_map(local, mesh=mesh, in_specs=in_specs, out_specs=P(("groups", "dp"), None), check_vma=False)
```

```python
import jax
import jax.numpy as jnp
from jax import lax
from jax.experimental import pallas as pl
from jax.experimental.pallas import tpu as pltpu
from jax.sharding import PartitionSpec as P

RANK = 64
BLOCK = 128
CORES = 2
TILE = 256

VMEM = pl.BlockSpec(memory_space=pltpu.VMEM)
SMEM = pl.BlockSpec(memory_space=pltpu.SMEM)
ANY = pl.BlockSpec(memory_space=pl.ANY)
LIMIT = 20 * 2**20


def side_by_side_kernel(left_ref, right_ref, whole_ref, top_ref, low_ref, sem):
    half, cut = top_ref.shape[0], left_ref.shape[1]
    copies = []
    for ref, rows in ((top_ref, slice(0, half)), (low_ref, slice(half, 2 * half)), (whole_ref, slice(0, 2 * half))):
        for source, columns in ((left_ref, slice(0, cut)), (right_ref, slice(cut, whole_ref.shape[1]))):
            copies.append(
                pltpu.make_async_copy(source.at[rows, :], ref.at[:, columns], sem.at[len(copies)])
            )
    for copy in copies:
        copy.start()
    for copy in copies:
        copy.wait()


def side_by_side(left, right):
    rows, width = left.shape[0], left.shape[1] + right.shape[1]
    whole = jax.ShapeDtypeStruct((rows, width), left.dtype)
    half = jax.ShapeDtypeStruct((rows // 2, width), left.dtype)
    return pl.pallas_call(
        side_by_side_kernel,
        out_shape=[whole, half, half],
        in_specs=[pl.BlockSpec(memory_space=pltpu.HBM)] * 2,
        out_specs=[VMEM] * 3,
        scratch_shapes=[pltpu.SemaphoreType.DMA((6,))],
        compiler_params=pltpu.CompilerParams(vmem_limit_bytes=LIMIT),
    )(left, right)


def stack_kernel(*refs):
    rows = refs[0].shape[0]
    for k, ref in enumerate(refs[:-1]):
        refs[-1][k * rows : (k + 1) * rows, :] = ref[...]


def stack(pieces):
    rows, width = pieces[0].shape
    return pl.pallas_call(
        stack_kernel,
        out_shape=jax.ShapeDtypeStruct((rows * len(pieces), width), pieces[0].dtype),
        in_specs=[VMEM] * len(pieces),
        out_specs=VMEM,
        compiler_params=pltpu.CompilerParams(vmem_limit_bytes=LIMIT),
        cost_estimate=pl.CostEstimate(flops=2**20, bytes_accessed=4 * rows * width * len(pieces), transcendentals=0),
    )(*pieces)


def accumulate_kernel(sources, part_count, first, chips, where_ref, tokens_ref, *refs):
    parts = refs[:part_count]
    acc_in = None if first else refs[part_count]
    out_ref, tok, sem = refs[part_count + (0 if first else 1) :]
    chip, sign, core = where_ref[0], where_ref[1], where_ref[2]
    copies = []
    for k, (distance, mine) in enumerate(sources):
        source = lax.rem(chip + sign * distance + chips, chips)
        side = lax.rem(core + distance + (0 if mine else 1), CORES)
        column = (source * CORES + side) * BLOCK
        copies.append(
            pltpu.make_async_copy(
                tokens_ref.at[:, pl.ds(pl.multiple_of(column, BLOCK), BLOCK)],
                tok.at[:, k * BLOCK : (k + 1) * BLOCK],
                sem.at[k],
            )
        )
    for copy in copies:
        copy.start()
    for copy in copies:
        copy.wait()

    def column_tile(k, carry):
        at = pl.ds(pl.multiple_of(k * TILE, TILE), TILE)
        total = None if first else acc_in[:, at]
        begin = 0
        for part in parts:
            end = begin + part.shape[0]
            term = jnp.dot(tok[:, begin:end], part[:, at], preferred_element_type=jnp.float32)
            total = term if total is None else total + term
            begin = end
        out_ref[:, at] = total.astype(out_ref.dtype)
        return carry

    lax.fori_loop(0, out_ref.shape[1] // TILE, column_tile, 0)


def accumulate(acc, tokens, where, chips, sources, parts, dtype=jnp.float32):
    rows, width = tokens.shape[0], parts[0].shape[1]
    first = acc is None
    n = len(sources)
    return pl.pallas_call(
        lambda *refs: accumulate_kernel(sources, len(parts), first, chips, *refs),
        out_shape=jax.ShapeDtypeStruct((rows, width), dtype),
        in_specs=[SMEM, ANY] + [VMEM] * (len(parts) + (0 if first else 1)),
        out_specs=VMEM,
        input_output_aliases={} if first or dtype != acc.dtype else {2 + len(parts): 0},
        scratch_shapes=[pltpu.VMEM((rows, n * BLOCK), jnp.bfloat16), pltpu.SemaphoreType.DMA((n,))],
        compiler_params=pltpu.CompilerParams(vmem_limit_bytes=LIMIT),
        cost_estimate=pl.CostEstimate(
            flops=2 * rows * n * BLOCK * width,
            bytes_accessed=2 * n * BLOCK * (rows + width) + 8 * rows * width,
            transcendentals=0,
        ),
    )(where, tokens, *parts, *([] if first else [acc]))


def finish_kernel(lengths_ref, ids_ref, scale_ref, acc_ref, got_ref, up_ref, out_ref):
    rows, cols = out_ref.shape
    deep = up_ref.shape[0]
    boundary = (lengths_ref[0] + BLOCK - 1) // BLOCK * BLOCK
    position = lax.broadcasted_iota(jnp.int32, (rows, 1), 0)
    second = position >= boundary
    offset = jnp.where(second, position - boundary, position)
    live = offset < jnp.where(second, lengths_ref[1], lengths_ref[0])
    adapter = jnp.where(second, ids_ref[1], ids_ref[0])
    scale = jnp.where(second, scale_ref[ids_ref[1]], scale_ref[ids_ref[0]])
    low = (acc_ref[:, cols:] + got_ref[:, cols:].astype(jnp.float32)).astype(jnp.bfloat16)
    owner = lax.broadcasted_iota(jnp.int32, (rows, deep), 1) // RANK
    wide = jnp.where(owner == adapter, low, jnp.zeros((), jnp.bfloat16))
    for k in range(cols // TILE):
        at = slice(k * TILE, (k + 1) * TILE)
        extra = jnp.dot(wide, up_ref[:, at], preferred_element_type=jnp.float32)
        base = acc_ref[:, at] + got_ref[:, at].astype(jnp.float32)
        out_ref[:, at] = jnp.where(live, base + scale * extra, 0.0).astype(out_ref.dtype)


def finish(acc, got, up, scale, lengths, ids):
    rows, width = acc.shape
    deep, cols = up.shape
    return pl.pallas_call(
        finish_kernel,
        out_shape=jax.ShapeDtypeStruct((rows, cols), jnp.bfloat16),
        in_specs=[SMEM, SMEM, SMEM, VMEM, VMEM, VMEM],
        out_specs=VMEM,
        compiler_params=pltpu.CompilerParams(vmem_limit_bytes=LIMIT),
        cost_estimate=pl.CostEstimate(flops=2 * rows * deep * cols, bytes_accessed=8 * rows * width, transcendentals=0),
    )(lengths, ids, scale, acc, got, up)


BATCHES = ((1, 2), (3, 5), (6, 8), (9, 10), (11, 12), (13, 14), (15, 15))
GROUPS = ((0,), (1,), (2,), (3, 4), (5, 6))


def solution(mesh):
    dp = mesh.shape["dp"]
    groups = mesh.shape["groups"]
    chips = dp // CORES
    far = chips // 2
    first_x = [d.coords[0] for d in mesh.devices[:, 0]]
    per_x = first_x.count(first_x[0])

    def parity(g):
        return (g // per_x + g % per_x) % 2

    def flat(g, z, c):
        return g * dp + z % chips * CORES + c

    places = [(g, z, c) for g in range(groups) for z in range(chips) for c in range(CORES)]
    forth = {(g, z, c): c == (parity(g) + z) % CORES for g, z, c in places}
    along = [(flat(*p), flat(p[0], p[1] + (1 if forth[p] else -1), 1 - p[2])) for p in places]
    across = [(flat(*p), flat(p[0] ^ per_x if forth[p] else p[0] ^ 1, p[1], 1 - p[2])) for p in places]
    mate = [(i, i ^ 1) for i in range(dp)]
    both = ("groups", "dp")

    def local(tokens, base_weight, down_stack, up_stack, adapter_scale, lengths, adapter_ids):
        place = lax.axis_index("dp")
        group = lax.axis_index("groups")
        chip, core = place // CORES, place % CORES
        sign = jnp.where(core == (parity(group) + chip) % CORES, -1, 1)
        where = jnp.stack([chip, sign, core]).astype(jnp.int32)
        own, a, b = side_by_side(base_weight, down_stack)
        theirs = lax.ppermute(tokens, "dp", mate)
        pieces = {}
        for s in range(1, far + 1):
            a = lax.ppermute(a, both, along)
            b = lax.ppermute(b, both, along)
            pieces[s] = [a, b]
        acc = acc_theirs = None
        for k, batches in enumerate(GROUPS):
            parts, sources = [], []
            for batch in batches:
                steps = range(BATCHES[batch][0], BATCHES[batch][1] + 1)
                near = stack([p for s in steps for p in pieces[s]])
                got = lax.ppermute(near, both, across)
                mine = [(s, True) for s in steps]
                if batch == len(BATCHES) - 1:
                    near = stack([p for s in (*steps, far) for p in pieces[s]])
                    mine.append((far, True))
                parts += [near, got]
                sources += mine + [(s, False) for s in steps]
            if k == 0:
                parts, sources = parts + [own], sources + [(0, True)]
            acc_theirs = accumulate(acc_theirs, theirs, where, chips, sources, parts)
            acc = accumulate(acc, tokens, where, chips, sources, parts)
        rest = lax.ppermute(acc_theirs, "dp", mate)
        return finish(acc, rest, up_stack, adapter_scale, lengths, adapter_ids)

    in_specs = (
        P(("groups", "dp"), None),
        P("dp", None),
        P("dp", None),
        P(),
        P(),
        P(("groups", "dp")),
        P(("groups", "dp")),
    )
    return jax.shard_map(local, mesh=mesh, in_specs=in_specs, out_specs=P(("groups", "dp"), None), check_vma=False)
```

```python
import jax
import jax.numpy as jnp
from jax import lax
from jax.experimental import pallas as pl
from jax.experimental.pallas import tpu as pltpu
from jax.sharding import PartitionSpec as P

RANK = 64
BLOCK = 128
CORES = 2
TILE = 256

VMEM = pl.BlockSpec(memory_space=pltpu.VMEM)
SMEM = pl.BlockSpec(memory_space=pltpu.SMEM)
ANY = pl.BlockSpec(memory_space=pl.ANY)
LIMIT = 20 * 2**20


def side_by_side_kernel(left_ref, right_ref, whole_ref, top_ref, low_ref, sem):
    half, cut = top_ref.shape[0], left_ref.shape[1]
    copies = []
    for ref, rows in ((top_ref, slice(0, half)), (low_ref, slice(half, 2 * half)), (whole_ref, slice(0, 2 * half))):
        for source, columns in ((left_ref, slice(0, cut)), (right_ref, slice(cut, whole_ref.shape[1]))):
            copies.append(
                pltpu.make_async_copy(source.at[rows, :], ref.at[:, columns], sem.at[len(copies)])
            )
    for copy in copies:
        copy.start()
    for copy in copies:
        copy.wait()


def side_by_side(left, right):
    rows, width = left.shape[0], left.shape[1] + right.shape[1]
    whole = jax.ShapeDtypeStruct((rows, width), left.dtype)
    half = jax.ShapeDtypeStruct((rows // 2, width), left.dtype)
    return pl.pallas_call(
        side_by_side_kernel,
        out_shape=[whole, half, half],
        in_specs=[pl.BlockSpec(memory_space=pltpu.HBM)] * 2,
        out_specs=[VMEM] * 3,
        scratch_shapes=[pltpu.SemaphoreType.DMA((6,))],
        compiler_params=pltpu.CompilerParams(vmem_limit_bytes=LIMIT),
    )(left, right)


def stack_kernel(*refs):
    rows = refs[0].shape[0]
    for k, ref in enumerate(refs[:-1]):
        refs[-1][k * rows : (k + 1) * rows, :] = ref[...]


def stack(pieces):
    rows, width = pieces[0].shape
    return pl.pallas_call(
        stack_kernel,
        out_shape=jax.ShapeDtypeStruct((rows * len(pieces), width), pieces[0].dtype),
        in_specs=[VMEM] * len(pieces),
        out_specs=VMEM,
        compiler_params=pltpu.CompilerParams(vmem_limit_bytes=LIMIT),
        cost_estimate=pl.CostEstimate(flops=2**20, bytes_accessed=4 * rows * width * len(pieces), transcendentals=0),
    )(*pieces)


def fetch(sources, chips, where_ref, tokens_ref, tok, sem):
    chip, sign, core = where_ref[0], where_ref[1], where_ref[2]
    copies = []
    for k, (distance, mine) in enumerate(sources):
        source = lax.rem(chip + sign * distance + chips, chips)
        side = lax.rem(core + distance + (0 if mine else 1), CORES)
        column = (source * CORES + side) * BLOCK
        copies.append(
            pltpu.make_async_copy(
                tokens_ref.at[:, pl.ds(pl.multiple_of(column, BLOCK), BLOCK)],
                tok.at[:, k * BLOCK : (k + 1) * BLOCK],
                sem.at[k],
            )
        )
    for copy in copies:
        copy.start()
    for copy in copies:
        copy.wait()


def gather(tokens, where, chips, sources):
    n = len(sources)
    return pl.pallas_call(
        lambda *refs: fetch(sources, chips, *refs),
        out_shape=jax.ShapeDtypeStruct((tokens.shape[0], n * BLOCK), tokens.dtype),
        in_specs=[SMEM, ANY],
        out_specs=VMEM,
        scratch_shapes=[pltpu.SemaphoreType.DMA((n,))],
        compiler_params=pltpu.CompilerParams(vmem_limit_bytes=LIMIT),
        cost_estimate=pl.CostEstimate(flops=2**20, bytes_accessed=4 * tokens.shape[0] * n * BLOCK, transcendentals=0),
    )(where, tokens)


def accumulate_kernel(sources, part_count, first, ready, chips, where_ref, tokens_ref, *refs):
    parts = refs[:part_count]
    acc_in = None if first else refs[part_count]
    out_ref, *scratch = refs[part_count + (0 if first else 1) :]
    tok = tokens_ref if ready else scratch[0]
    if not ready:
        fetch(sources, chips, where_ref, tokens_ref, *scratch)

    def column_tile(k, carry):
        at = pl.ds(pl.multiple_of(k * TILE, TILE), TILE)
        total = None if first else acc_in[:, at]
        begin = 0
        for part in parts:
            end = begin + part.shape[0]
            term = jnp.dot(tok[:, begin:end], part[:, at], preferred_element_type=jnp.float32)
            total = term if total is None else total + term
            begin = end
        out_ref[:, at] = total.astype(out_ref.dtype)
        return carry

    lax.fori_loop(0, out_ref.shape[1] // TILE, column_tile, 0)


def accumulate(acc, tokens, where, chips, sources, parts, ready=False):
    rows, width = tokens.shape[0], parts[0].shape[1]
    first = acc is None
    n = len(sources)
    return pl.pallas_call(
        lambda *refs: accumulate_kernel(sources, len(parts), first, ready, chips, *refs),
        out_shape=jax.ShapeDtypeStruct((rows, width), jnp.float32),
        in_specs=[SMEM, VMEM if ready else ANY] + [VMEM] * (len(parts) + (0 if first else 1)),
        out_specs=VMEM,
        input_output_aliases={} if first else {2 + len(parts): 0},
        scratch_shapes=[]
        if ready
        else [pltpu.VMEM((rows, n * BLOCK), jnp.bfloat16), pltpu.SemaphoreType.DMA((n,))],
        compiler_params=pltpu.CompilerParams(vmem_limit_bytes=LIMIT),
        cost_estimate=pl.CostEstimate(
            flops=2 * rows * n * BLOCK * width,
            bytes_accessed=2 * n * BLOCK * (rows + width) + 8 * rows * width,
            transcendentals=0,
        ),
    )(where, tokens, *parts, *([] if first else [acc]))


def finish_kernel(lengths_ref, ids_ref, scale_ref, acc_ref, got_ref, up_ref, out_ref):
    rows, cols = out_ref.shape
    deep = up_ref.shape[0]
    boundary = (lengths_ref[0] + BLOCK - 1) // BLOCK * BLOCK
    position = lax.broadcasted_iota(jnp.int32, (rows, 1), 0)
    second = position >= boundary
    offset = jnp.where(second, position - boundary, position)
    live = offset < jnp.where(second, lengths_ref[1], lengths_ref[0])
    adapter = jnp.where(second, ids_ref[1], ids_ref[0])
    scale = jnp.where(second, scale_ref[ids_ref[1]], scale_ref[ids_ref[0]])
    low = (acc_ref[:, cols:] + got_ref[:, cols:].astype(jnp.float32)).astype(jnp.bfloat16)
    owner = lax.broadcasted_iota(jnp.int32, (rows, deep), 1) // RANK
    wide = jnp.where(owner == adapter, low, jnp.zeros((), jnp.bfloat16))
    for k in range(cols // TILE):
        at = slice(k * TILE, (k + 1) * TILE)
        extra = jnp.dot(wide, up_ref[:, at], preferred_element_type=jnp.float32)
        base = acc_ref[:, at] + got_ref[:, at].astype(jnp.float32)
        out_ref[:, at] = jnp.where(live, base + scale * extra, 0.0).astype(out_ref.dtype)


def finish(acc, got, up, scale, lengths, ids):
    rows, width = acc.shape
    deep, cols = up.shape
    return pl.pallas_call(
        finish_kernel,
        out_shape=jax.ShapeDtypeStruct((rows, cols), jnp.bfloat16),
        in_specs=[SMEM, SMEM, SMEM, VMEM, VMEM, VMEM],
        out_specs=VMEM,
        compiler_params=pltpu.CompilerParams(vmem_limit_bytes=LIMIT),
        cost_estimate=pl.CostEstimate(flops=2 * rows * deep * cols, bytes_accessed=8 * rows * width, transcendentals=0),
    )(lengths, ids, scale, acc, got, up)


BATCHES = ((1, 2), (3, 5), (6, 8), (9, 10), (11, 12), (13, 14), (15, 15))
GROUPS = ((0,), (1,), (2,), (3, 4), (5, 6))


def solution(mesh):
    dp = mesh.shape["dp"]
    groups = mesh.shape["groups"]
    chips = dp // CORES
    far = chips // 2
    first_x = [d.coords[0] for d in mesh.devices[:, 0]]
    per_x = first_x.count(first_x[0])

    def parity(g):
        return (g // per_x + g % per_x) % 2

    def flat(g, z, c):
        return g * dp + z % chips * CORES + c

    places = [(g, z, c) for g in range(groups) for z in range(chips) for c in range(CORES)]
    forth = {(g, z, c): c == (parity(g) + z) % CORES for g, z, c in places}
    along = [(flat(*p), flat(p[0], p[1] + (1 if forth[p] else -1), 1 - p[2])) for p in places]
    across = [(flat(*p), flat(p[0] ^ per_x if forth[p] else p[0] ^ 1, p[1], 1 - p[2])) for p in places]
    mate = [(i, i ^ 1) for i in range(dp)]
    both = ("groups", "dp")

    def local(tokens, base_weight, down_stack, up_stack, adapter_scale, lengths, adapter_ids):
        place = lax.axis_index("dp")
        group = lax.axis_index("groups")
        chip, core = place // CORES, place % CORES
        sign = jnp.where(core == (parity(group) + chip) % CORES, -1, 1)
        where = jnp.stack([chip, sign, core]).astype(jnp.int32)
        own, a, b = side_by_side(base_weight, down_stack)
        theirs = lax.ppermute(tokens, "dp", mate)
        pieces = {}
        for s in range(1, far + 1):
            a = lax.ppermute(a, both, along)
            b = lax.ppermute(b, both, along)
            pieces[s] = [a, b]
        acc = acc_theirs = None
        for k, batches in enumerate(GROUPS):
            parts, sources = [], []
            for batch in batches:
                steps = range(BATCHES[batch][0], BATCHES[batch][1] + 1)
                near = stack([p for s in steps for p in pieces[s]])
                got = lax.ppermute(near, both, across)
                mine = [(s, True) for s in steps]
                if batch == len(BATCHES) - 1:
                    near = stack([p for s in (*steps, far) for p in pieces[s]])
                    mine.append((far, True))
                parts += [near, got]
                sources += mine + [(s, False) for s in steps]
            if k == 0:
                parts, sources = parts + [own], sources + [(0, True)]
            final = k == len(GROUPS) - 1
            if final:
                theirs = gather(theirs, where, chips, sources)
            acc_theirs = accumulate(acc_theirs, theirs, where, chips, sources, parts, final)
            acc = accumulate(acc, tokens, where, chips, sources, parts)
        rest = lax.ppermute(acc_theirs, "dp", mate)
        return finish(acc, rest, up_stack, adapter_scale, lengths, adapter_ids)

    in_specs = (
        P(("groups", "dp"), None),
        P("dp", None),
        P("dp", None),
        P(),
        P(),
        P(("groups", "dp")),
        P(("groups", "dp")),
    )
    return jax.shard_map(local, mesh=mesh, in_specs=in_specs, out_specs=P(("groups", "dp"), None), check_vma=False)
```
